32 devices in a mesh: task: 8 (over z, y), aux: 4 (over x, core).
Axes of the slice: x: 2, y: 2, z: 4, core: 2. Of those that a mesh axis runs over, the one named last changes fastest.
Arguments:
- factors: bfloat16 [8, 2048, 1024], P('task', 'aux'), may hold values from -0.125 to 0.125
- amplitudes: bfloat16 [8, 256, 1024], P('task'), may hold values from -6 to 6
- task_counts: int32 [8], P('task'), may hold values from 1 to 4, 16 in all
- task_tiles: int32 [8, 4, 3], P('task'), may hold values from 0 to 4
Outputs:
- residual: float32 [8, 256, 1024], P('task', None, 'aux')
The draws below stay inside these ranges and needn't reach their ends.
Inputs may be any that keep to these rules, and one draw needn't show every extreme that they name: `task_counts`: every tile has 1 to 4 tasks, exactly 16 in all; some tile has exactly 4.
All inputs are finite; a program needn't handle non-finite values. No bound on the sum of `task_counts` on one device may be relied on, other than what follows from the above.
Results may differ from the reference program's by a relative error of at most 0.0026.
Values may be sent and summed in bfloat16 or wider, within the bound.
A program may use at most 64 MiB of HBM per device.

```python
import math
import jax
import jax.numpy as jnp
import numpy as np
from jax import lax

AUX = 2048
VB = 32
PAIRS = 1024
OCCP = 256
MOST = 4
RADIUS = 2
TILES = 8
TASKS = 16
N_AUX = 4


def place_ends(result, stream_key, smallest, top_value):
    index_at = [jax.random.randint(jax.random.fold_in(stream_key, axis), (), 0, length) for axis, length in enumerate(result.shape)]
    widest = result.shape.index(max(result.shape))
    neighbour = index_at[:widest] + [(index_at[widest] + 1) % result.shape[widest]] + index_at[widest + 1:]
    return result.at[tuple(index_at)].set(smallest).at[tuple(neighbour)].set(top_value)


def steps_of(key, dims, cuts, smallest, top_value):
    gain, own = 1.0, jax.random.fold_in(key, 6)
    for position, shards_of in cuts:
        steps = jnp.exp(jax.random.uniform(jax.random.fold_in(own, position), (shards_of,), jnp.float32, smallest / len(cuts), top_value / len(cuts)))
        gain = gain * jnp.repeat(steps, dims[position] // shards_of).reshape([-1 if axis == position else 1 for axis in range(len(dims))])
    return gain


def profile(count, total, bound, slope):
    weights = [(1 << 20) // math.isqrt(grade ** slope) + 1 for grade in range(2, count + 1)]
    rest, counts = total - bound - (count - 1), [1] * (count - 1)
    while rest > 0:
        movable = [i for i in range(count - 1) if counts[i] < bound]
        pool, remaining = sum([weights[i] for i in movable]), rest
        for i in movable:
            addition = min(bound - counts[i], max(1, remaining * weights[i] // pool), rest)
            counts[i] = counts[i] + addition
            rest = rest - addition
    return np.array([bound] + counts)


def uneven(stream_key, amount, total, bound, skew):
    if amount == 2:
        one = jax.random.randint(stream_key, (), max(1, total - bound), min(bound, total - 1) + 1)
        return jnp.stack([one, total - one])
    tallies = jnp.asarray(profile(amount, total, bound, skew), jnp.int32)
    pairs = (amount - 1) // 2
    giver, sink = tallies[1:1 + 2 * pairs:2], tallies[2:2 + 2 * pairs:2]
    margin = jnp.minimum(giver - 1, bound - sink)
    moved = jax.random.randint(jax.random.fold_in(stream_key, 1), (pairs,), 0, 1 << 20) % (margin + 1)
    tallies = tallies.at[1:1 + 2 * pairs:2].set(giver - moved).at[2:2 + 2 * pairs:2].set(sink + moved)
    return tallies[jax.random.permutation(jax.random.fold_in(stream_key, 2), amount)]


def gaussian(own_key, dims, spread, reach, shards=(), kind=jnp.bfloat16):
    result = jax.random.normal(own_key, dims, jnp.float32) * spread
    if len(shards) > 0:
        result = steps_of(own_key, dims, shards, -0.22, 0.18) * result
    return jnp.clip(result, min=-reach, max=reach).astype(kind)


def setup_inputs(seed: int = 0) -> dict:
    seeds = jax.random.split(jax.random.key(seed), 5)
    return {
        "factors": gaussian(seeds[0], (TILES, AUX, PAIRS), AUX ** -0.5, 0.125, ((0, 8), (1, 4))),
        "amplitudes": gaussian(seeds[1], (TILES, OCCP, PAIRS), 1.0, 6.0, ((0, 8),)),
        "task_counts": uneven(seeds[2], TILES, TASKS, MOST, 2).astype(jnp.int32),
        "task_tiles": place_ends(jax.random.randint(seeds[3], (TILES, MOST, 3), 0, 2 * RADIUS + 1), jax.random.fold_in(seeds[3], 1), 0, 2 * RADIUS).astype(jnp.int32),
    }


def quarter_term(first, second, amp):
    tile = lax.dot_general(first, second, (((0,), (0,)), ((), ())), preferred_element_type=jnp.float32)
    tile = tile.reshape(VB, VB, VB, VB).transpose(1, 3, 0, 2).reshape(VB * VB, VB * VB)
    tile = tile.astype(jnp.bfloat16)
    return jnp.dot(amp, tile, preferred_element_type=jnp.float32)


def task_term(first, second, amp):
    width = AUX // N_AUX
    total = jnp.zeros((amp.shape[0], VB * VB), jnp.float32)
    for quarter in range(N_AUX):
        lower = quarter * width
        total = total + quarter_term(first[lower:lower + width], second[lower:lower + width], amp)
    return total


def reference(factors, amplitudes, task_counts, task_tiles):
    owners = jnp.repeat(jnp.arange(TILES, dtype=jnp.int32), MOST)
    slots = jnp.tile(jnp.arange(MOST, dtype=jnp.int32), TILES)

    def step(total, item):
        owner, slot = item
        offs = task_tiles[owner, slot]
        idx = (owner + offs - RADIUS) % TILES
        live = slot < task_counts[owner]

        def compute(unused):
            return task_term(factors[idx[0]], factors[idx[1]], amplitudes[idx[2]])

        def empty(unused):
            return jnp.zeros((OCCP, VB * VB), jnp.float32)

        term = lax.cond(live, compute, empty, 0)
        total = lax.dynamic_update_index_in_dim(total, lax.dynamic_index_in_dim(total, owner, 0, False) + term, owner, 0)
        return total, 0

    start = jnp.zeros((TILES, OCCP, VB * VB), jnp.float32)
    total, unused = lax.scan(step, start, (owners, slots))
    return total
```

```python
import functools

import jax
import jax.numpy as jnp
from jax import lax
from jax.experimental import pallas as pl
from jax.experimental.pallas import tpu as pltpu
from jax.sharding import PartitionSpec as P

VB = 32
RADIUS = 2
SPAN = 2 * RADIUS + 1
MOST = 4
LANES = 128
SPREAD = LANES // VB
STEP = 2
N_AUX = 4
MESH = pl.DeviceIdType.MESH


def roll_groups(x, amount):
    if amount == 0:
        return x
    parts = [
        pltpu.roll(x[:, j * LANES : (j + 1) * LANES], amount, 1)
        for j in range(x.shape[1] // LANES)
    ]
    return jnp.concatenate(parts, axis=1)


def cut_rows(depth):
    groups = []
    blocks = depth // LANES
    for b in range(blocks):
        lo = b * LANES
        if b == blocks - 1:
            half = LANES // 2
            groups.append([(lo, half), (lo + half, half)])
        else:
            groups.append([(lo, LANES)])
    return groups


def kernel(
    n_task,
    relayed,
    counts,
    plan,
    fac_in,
    amp_in,
    out,
    fac,
    amp,
    ampt,
    lt,
    right,
    tile,
    swap,
    part,
    inbox,
    xsend,
    xin,
    local_sem,
    fsend,
    frecv,
    tsend,
    trecv,
    qsend,
    qrecv,
    csend,
    crecv,
):
    depth, pairs = fac_in.shape
    occ = amp_in.shape[0]
    share = occ // N_AUX
    blocks = pairs // LANES
    width = pairs // N_AUX
    lanes = STEP * LANES
    t = lax.axis_index("task")
    k = lax.axis_index("aux")
    mate = t + 1 - 2 * (t % 2)
    odd = t % 2

    def aux_peer(bits):
        flip_low = bits % 2
        flip_high = bits // 2
        low = k % 2
        high = k // 2
        if flip_low:
            low = 1 - low
        if flip_high:
            high = 1 - high
        return high * 2 + low

    def wrapped(d):
        return lax.rem(t + d + n_task, n_task)

    if relayed:
        paths = [(wrapped(2), 0), (wrapped(-2), 4), (mate, 1 + 2 * odd)]
        early = [0, 4]
        direct = 3 - 2 * odd
        late = 1 + 2 * odd
        relay_from = 4 - 4 * odd
        relay_to = 3 - 2 * odd
    else:
        paths = [(wrapped(2), 0), (wrapped(-2), 4), (wrapped(1), 1), (wrapped(-1), 3)]
        early = [0, 4]
        direct = 1
        late = 3

    barrier = pltpu.get_barrier_semaphore()
    for peer, _ in paths:
        pl.semaphore_signal(barrier, inc=1, device_id={"task": peer}, device_id_type=MESH)
    for bits in range(1, N_AUX):
        pl.semaphore_signal(
            barrier, inc=1, device_id={"aux": aux_peer(bits)}, device_id_type=MESH
        )
    own_f = pltpu.make_async_copy(fac_in, fac.at[RADIUS], local_sem.at[0])
    own_t = pltpu.make_async_copy(amp_in, amp.at[RADIUS], local_sem.at[1])
    own_f.start()
    own_t.start()
    pl.semaphore_wait(barrier, len(paths) + N_AUX - 1)

    groups = cut_rows(depth)
    pieces = [piece for group in groups for piece in group]
    mine = pl.ds(pl.multiple_of(k * share, share), share)

    def send_piece(i, path, peer, src, slot):
        lo, size = pieces[i]
        return pltpu.make_async_remote_copy(
            src_ref=src.at[pl.ds(lo, size)],
            dst_ref=fac.at[slot, pl.ds(lo, size)],
            send_sem=fsend.at[path, i],
            recv_sem=frecv.at[slot, i],
            device_id={"task": peer},
            device_id_type=MESH,
        )

    def send_amp(path, peer, src, slot):
        return pltpu.make_async_remote_copy(
            src_ref=src,
            dst_ref=amp.at[slot, mine],
            send_sem=tsend.at[path],
            recv_sem=trecv.at[slot],
            device_id={"task": peer},
            device_id_type=MESH,
        )

    def spread_amp(slot, order, bits):
        return pltpu.make_async_remote_copy(
            src_ref=amp.at[slot, mine],
            dst_ref=amp.at[slot, mine],
            send_sem=qsend.at[order, bits - 1],
            recv_sem=qrecv.at[slot, bits - 1],
            device_id={"aux": aux_peer(bits)},
            device_id_type=MESH,
        )

    started = []

    def start(copy):
        copy.start()
        started.append(copy)

    for path, (peer, slot) in enumerate(paths):
        start(send_amp(path, peer, amp_in.at[mine], slot))
    for i in range(len(pieces)):
        for path, (peer, slot) in enumerate(paths):
            start(send_piece(i, path, peer, fac_in, slot))

    @pl.loop(0, blocks)
    def _(j):
        base = pl.multiple_of(j * LANES, LANES)
        rows = lax.broadcasted_iota(jnp.int32, (LANES, pairs), 0) + base
        cols = lax.broadcasted_iota(jnp.int32, (LANES, pairs), 1)
        hit = rows == (cols % VB) * VB + cols // VB
        swap[pl.ds(base, LANES), :] = hit.astype(jnp.float32).astype(jnp.bfloat16)

    def prepare(slot, b):
        span = pl.ds(b * LANES, LANES)
        x = fac[slot, span, :]
        for hi in range(blocks):
            strip = x[:, hi * LANES : (hi + 1) * LANES].T
            for s in range(SPREAD):
                lt[slot, s, hi * VB : (hi + 1) * VB, span] = strip[s * VB : (s + 1) * VB, :]
        swapped = jnp.dot(x, swap[...], preferred_element_type=jnp.float32)
        for s in range(SPREAD):
            right[slot, s, span, :] = roll_groups(swapped, s * VB).astype(jnp.bfloat16)

    def prepare_amp(slot):
        ampt[slot] = jnp.dot(
            amp[slot], swap[...], preferred_element_type=jnp.float32
        ).astype(jnp.bfloat16)

    def amp_arrived(slot, order):
        send_amp(0, t, amp_in.at[mine], slot).wait_recv()
        for bits in range(1, N_AUX):
            start(spread_amp(slot, order, bits))

    def amp_ready(slot, order):
        for bits in range(1, N_AUX):
            spread_amp(slot, order, bits).wait_recv()
        prepare_amp(slot)

    def arrived(slot, i):
        send_piece(i, 0, t, fac_in, slot).wait_recv()

    own_t.wait()
    own_f.wait()
    prepare_amp(RADIUS)
    for b in range(len(groups)):
        prepare(RADIUS, b)

    for order, slot in enumerate(early):
        amp_arrived(slot, order)
    if relayed:
        start(send_amp(3, mate, amp.at[relay_from, mine], relay_to))
    amp_arrived(direct, 2)

    first = 0
    for b, group in enumerate(groups):
        for i in range(first, first + len(group)):
            for slot in early:
                arrived(slot, i)
            if relayed:
                start(send_piece(i, 3, mate, fac.at[relay_from], relay_to))
        if b > 0:
            previous = len(groups[b - 1])
            for i in range(first - previous, first):
                arrived(late, i)
            prepare(late, b - 1)
        for i in range(first, first + len(group)):
            arrived(direct, i)
        for slot in early + [direct]:
            prepare(slot, b)
        if b == 0:
            amp_arrived(late, 3)
            for order, slot in enumerate(early):
                amp_ready(slot, order)
        if b == 1:
            amp_ready(direct, 2)
            amp_ready(late, 3)
        first += len(group)
    for i in range(first - len(groups[-1]), first):
        arrived(late, i)
    prepare(late, len(groups) - 1)

    half_rows = blocks * VB
    group_of = (lax.broadcasted_iota(jnp.int32, (half_rows, lanes), 1) // VB) % SPREAD

    @pl.loop(0, MOST)
    def _(slot):
        left_tile, right_tile = plan[0, 0, slot], plan[1, 0, slot]

        @pl.loop(0, blocks // STEP)
        def _(step):
            base = pl.multiple_of(step * lanes, lanes)
            outs = [
                jnp.dot(
                    lt[left_tile, s],
                    right[right_tile, s, :, pl.ds(base, lanes)],
                    preferred_element_type=jnp.float32,
                )
                for s in range(SPREAD)
            ]
            for d in range(SPREAD):
                mixed = outs[(SPREAD - 1 - d) % SPREAD]
                for g in range(SPREAD - 1):
                    mixed = jnp.where(group_of == g, outs[(g - d) % SPREAD], mixed)
                mixed = roll_groups(mixed, (LANES - d * VB) % LANES).astype(jnp.bfloat16)
                for j in range(STEP):
                    row = pl.multiple_of(base + (j * SPREAD + d) * VB, VB)
                    for hi in range(blocks):
                        tile[slot, pl.ds(row, VB), hi * LANES : (hi + 1) * LANES] = mixed[
                            hi * VB : (hi + 1) * VB, j * LANES : (j + 1) * LANES
                        ]

    low = k % 2
    high = k // 2

    def swap_sums(stage, bits, src, dst):
        return pltpu.make_async_remote_copy(
            src_ref=src,
            dst_ref=dst,
            send_sem=csend.at[stage],
            recv_sem=crecv.at[stage],
            device_id={"aux": aux_peer(bits)},
            device_id_type=MESH,
        )

    for stage, side in enumerate((1 - high, high)):
        cols = pl.ds(pl.multiple_of(side * 2 * width, 2 * width), 2 * width)
        total = jnp.zeros((occ, 2 * width), jnp.float32)
        for slot in range(MOST):
            term = jnp.dot(
                ampt[plan[2, 0, slot]], tile[slot, :, cols], preferred_element_type=jnp.float32
            )
            total += jnp.where(slot < counts[0], term, 0.0)
        part[stage, 0] = total[:, :width]
        part[stage, 1] = total[:, width:]
        pair = swap_sums(stage, 1, part.at[stage, 1 - low], inbox.at[stage])
        start(pair)
        if stage == 0:
            pair.wait_recv()
            xsend[...] = part[stage, low] + inbox[stage]
            far = swap_sums(2, 2, xsend, xin)
            start(far)
        else:
            pair.wait_recv()
            far.wait_recv()
            out[...] = part[stage, low] + inbox[stage] + xin[...]

    for copy in started:
        copy.wait_send()


def run(factors, amplitudes, counts, plan, n_task, relayed):
    depth, pairs = factors.shape
    occ = amplitudes.shape[0]
    width = pairs // N_AUX
    n_pieces = sum(len(group) for group in cut_rows(depth))
    anywhere = pl.BlockSpec(memory_space=pl.ANY)
    scalars = pl.BlockSpec(memory_space=pltpu.SMEM)
    dma = pltpu.SemaphoreType.DMA
    return pl.pallas_call(
        functools.partial(kernel, n_task, relayed),
        out_shape=jax.ShapeDtypeStruct((occ, width), jnp.float32),
        in_specs=[scalars, scalars, anywhere, anywhere],
        out_specs=pl.BlockSpec(memory_space=pltpu.VMEM),
        scratch_shapes=[
            pltpu.VMEM((SPAN, depth, pairs), jnp.bfloat16),
            pltpu.VMEM((SPAN, occ, pairs), jnp.bfloat16),
            pltpu.VMEM((SPAN, occ, pairs), jnp.bfloat16),
            pltpu.VMEM((SPAN, SPREAD, pairs // SPREAD, depth), jnp.bfloat16),
            pltpu.VMEM((SPAN, SPREAD, depth, pairs), jnp.bfloat16),
            pltpu.VMEM((MOST, pairs, pairs), jnp.bfloat16),
            pltpu.VMEM((pairs, pairs), jnp.bfloat16),
            pltpu.VMEM((2, 2, occ, width), jnp.float32),
            pltpu.VMEM((2, occ, width), jnp.float32),
            pltpu.VMEM((occ, width), jnp.float32),
            pltpu.VMEM((occ, width), jnp.float32),
            dma((2,)),
            dma((4, n_pieces)),
            dma((SPAN, n_pieces)),
            dma((4,)),
            dma((SPAN,)),
            dma((4, N_AUX - 1)),
            dma((SPAN, N_AUX - 1)),
            dma((3,)),
            dma((3,)),
        ],
        compiler_params=pltpu.CompilerParams(
            vmem_limit_bytes=60 * 1024 * 1024, collective_id=0, has_side_effects=True
        ),
    )(counts, plan, factors, amplitudes)


def solution(mesh):
    n_task, n_aux = mesh.shape["task"], mesh.shape["aux"]
    assert n_aux == N_AUX
    relayed = n_task == 8

    def shards(factors, amplitudes, task_counts, task_tiles):
        plan = jnp.transpose(task_tiles, (2, 0, 1))
        total = run(factors[0], amplitudes[0], task_counts, plan, n_task, relayed)
        return total[None]

    return jax.shard_map(
        shards,
        mesh=mesh,
        in_specs=(P("task", "aux", None), P("task", None, None), P("task"), P("task", None, None)),
        out_specs=P("task", None, "aux"),
        check_vma=False,
    )
```

```python
import functools

import jax
import jax.numpy as jnp
from jax import lax
from jax.experimental import pallas as pl
from jax.experimental.pallas import tpu as pltpu
from jax.sharding import PartitionSpec as P

VB = 32
RADIUS = 2
SPAN = 2 * RADIUS + 1
MOST = 4
LANES = 128
SPREAD = LANES // VB
STEP = 2
N_AUX = 4
TRIGGER = 2
MESH = pl.DeviceIdType.MESH


def roll_groups(x, amount):
    if amount == 0:
        return x
    parts = [
        pltpu.roll(x[:, j * LANES : (j + 1) * LANES], amount, 1)
        for j in range(x.shape[1] // LANES)
    ]
    return jnp.concatenate(parts, axis=1)


def cut_rows(depth):
    groups = []
    blocks = depth // LANES
    for b in range(blocks):
        lo = b * LANES
        if b == blocks - 1:
            half = LANES // 2
            groups.append([(lo, half), (lo + half, half)])
        else:
            groups.append([(lo, LANES)])
    return groups


def kernel(
    n_task,
    relayed,
    counts,
    plan,
    fac_in,
    amp_in,
    out,
    fac,
    amp,
    ampt,
    lt,
    right,
    vacc,
    swap,
    part,
    inbox,
    xsend,
    xin,
    local_sem,
    fsend,
    frecv,
    tsend,
    trecv,
    qsend,
    qrecv,
    csend,
    crecv,
):
    depth, pairs = fac_in.shape
    occ = amp_in.shape[0]
    share = occ // N_AUX
    blocks = pairs // LANES
    width = pairs // N_AUX
    lanes = STEP * LANES
    t = lax.axis_index("task")
    k = lax.axis_index("aux")
    mate = t + 1 - 2 * (t % 2)
    odd = t % 2

    def aux_peer(bits):
        flip_low = bits % 2
        flip_high = bits // 2
        low = k % 2
        high = k // 2
        if flip_low:
            low = 1 - low
        if flip_high:
            high = 1 - high
        return high * 2 + low

    def wrapped(d):
        return lax.rem(t + d + n_task, n_task)

    if relayed:
        paths = [
            (wrapped(4 * odd - 2), 4 - 4 * odd),
            (mate, 1 + 2 * odd),
            (wrapped(2 - 4 * odd), 4 * odd),
        ]
        ahead, near, behind, late = 4 - 4 * odd, 3 - 2 * odd, 4 * odd, 1 + 2 * odd
        relay_to = 3 - 2 * odd
    else:
        paths = [(wrapped(2), 0), (wrapped(-1), 3), (wrapped(-2), 4), (wrapped(1), 1)]
        ahead, near, behind, late = 0, 3, 4, 1

    barrier = pltpu.get_barrier_semaphore()
    for peer, _ in paths:
        pl.semaphore_signal(barrier, inc=1, device_id={"task": peer}, device_id_type=MESH)
    for bits in range(1, N_AUX):
        pl.semaphore_signal(
            barrier, inc=1, device_id={"aux": aux_peer(bits)}, device_id_type=MESH
        )
    own_f = pltpu.make_async_copy(fac_in, fac.at[RADIUS], local_sem.at[0])
    own_t = pltpu.make_async_copy(amp_in, amp.at[RADIUS], local_sem.at[1])
    own_f.start()
    own_t.start()
    pl.semaphore_wait(barrier, len(paths) + N_AUX - 1)

    groups = cut_rows(depth)
    pieces = [piece for group in groups for piece in group]
    held = depth // 2
    mine = pl.ds(pl.multiple_of(k * share, share), share)

    def send_piece(i, path, peer, src, slot):
        lo, size = pieces[i]
        return pltpu.make_async_remote_copy(
            src_ref=src.at[pl.ds(lo, size)],
            dst_ref=fac.at[slot, pl.ds(lo, size)],
            send_sem=fsend.at[path, i],
            recv_sem=frecv.at[slot, i],
            device_id={"task": peer},
            device_id_type=MESH,
        )

    def send_amp(path, peer, src, slot):
        return pltpu.make_async_remote_copy(
            src_ref=src,
            dst_ref=amp.at[slot, mine],
            send_sem=tsend.at[path],
            recv_sem=trecv.at[slot],
            device_id={"task": peer},
            device_id_type=MESH,
        )

    def spread_amp(slot, order, bits):
        return pltpu.make_async_remote_copy(
            src_ref=amp.at[slot, mine],
            dst_ref=amp.at[slot, mine],
            send_sem=qsend.at[order, bits - 1],
            recv_sem=qrecv.at[slot, bits - 1],
            device_id={"aux": aux_peer(bits)},
            device_id_type=MESH,
        )

    started = []

    def start(copy):
        copy.start()
        started.append(copy)

    def send_own(path):
        peer, slot = paths[path]
        for i in range(len(pieces)):
            start(send_piece(i, path, peer, fac_in, slot))

    for path, (peer, slot) in enumerate(paths):
        start(send_amp(path, peer, amp_in.at[mine], slot))
    send_own(0)
    send_own(1)
    if not relayed:
        send_own(2)
        send_own(3)

    @pl.loop(0, blocks)
    def _(j):
        base = pl.multiple_of(j * LANES, LANES)
        rows = lax.broadcasted_iota(jnp.int32, (LANES, pairs), 0) + base
        cols = lax.broadcasted_iota(jnp.int32, (LANES, pairs), 1)
        hit = rows == (cols % VB) * VB + cols // VB
        swap[pl.ds(base, LANES), :] = hit.astype(jnp.float32).astype(jnp.bfloat16)

    def prepare(slot, b):
        x = fac[slot, pl.ds(b * LANES, LANES), :]
        part_of, lo = b * LANES // held, b * LANES % held
        span = pl.ds(lo, LANES)
        for hi in range(blocks):
            strip = x[:, hi * LANES : (hi + 1) * LANES].T
            for s in range(SPREAD):
                lt[part_of, slot, s, hi * VB : (hi + 1) * VB, span] = strip[
                    s * VB : (s + 1) * VB, :
                ]
        swapped = jnp.dot(x, swap[...], preferred_element_type=jnp.float32)
        for s in range(SPREAD):
            right[part_of, slot, s, span, :] = roll_groups(swapped, s * VB).astype(jnp.bfloat16)

    def prepare_amp(slot):
        ampt[slot] = jnp.dot(
            amp[slot], swap[...], preferred_element_type=jnp.float32
        ).astype(jnp.bfloat16)

    def amp_arrived(slot, order):
        send_amp(0, t, amp_in.at[mine], slot).wait_recv()
        for bits in range(1, N_AUX):
            start(spread_amp(slot, order, bits))

    def amp_ready(slot):
        for bits in range(1, N_AUX):
            spread_amp(slot, 0, bits).wait_recv()
        prepare_amp(slot)

    def arrived(slot, i):
        send_piece(i, 0, t, fac_in, slot).wait_recv()

    own_t.wait()
    own_f.wait()
    prepare_amp(RADIUS)
    for b in range(len(groups)):
        prepare(RADIUS, b)

    amp_arrived(ahead, 0)
    if relayed:
        start(send_amp(3, mate, amp.at[ahead, mine], relay_to))
    amp_arrived(near, 1)
    amp_arrived(behind, 2)

    i = 0
    for b, group in enumerate(groups):
        for _ in group:
            arrived(ahead, i)
            if relayed:
                start(send_piece(i, 3, mate, fac.at[ahead], relay_to))
                if i == len(pieces) - TRIGGER:
                    send_own(2)
            i += 1
        prepare(ahead, b)
        for j in range(i - len(group), i):
            arrived(near, j)
        prepare(near, b)
        if b == 0:
            amp_arrived(late, 3)
        if b == 1:
            for slot in (ahead, near, behind, late):
                amp_ready(slot)

    lane_blocks = blocks // STEP

    def product(part_of, slot, s, cols):
        return jnp.dot(
            lt[part_of, plan[0, 0, slot], s],
            right[part_of, plan[1, 0, slot], s, :, cols],
            preferred_element_type=jnp.float32,
        )

    i = 0
    for b, group in enumerate(groups):
        for slot in (behind, late):
            for j in range(i, i + len(group)):
                arrived(slot, j)
            prepare(slot, b)
        i += len(group)
        if (b + 1) * LANES == held:

            @pl.loop(0, MOST)
            def _(slot):
                @pl.loop(0, lane_blocks)
                def _(step):
                    cols = pl.ds(pl.multiple_of(step * lanes, lanes), lanes)
                    for s in range(SPREAD):
                        vacc[slot, s, :, cols] = product(0, slot, s, cols)

    flat = right.at[0]
    group_of = (lax.broadcasted_iota(jnp.int32, (blocks * VB, LANES), 1) // VB).astype(
        jnp.float32
    )
    is_odd = (group_of == 1.0) | (group_of == 3.0)
    is_high = group_of >= 2.0

    @pl.loop(0, MOST)
    def _(slot):
        @pl.loop(0, lane_blocks)
        def _(step):
            cols = pl.ds(pl.multiple_of(step * lanes, lanes), lanes)
            for s in range(SPREAD):
                whole = vacc[slot, s, :, cols] + product(1, slot, s, cols)
                flat[MOST, s, :, cols] = whole.astype(jnp.bfloat16)

        for db in range(blocks):
            x = [flat[MOST, s, :, db * LANES : (db + 1) * LANES] for s in range(SPREAD)]
            p = [jnp.where(is_odd, x[(j + 1) % SPREAD], x[j]) for j in range(SPREAD)]
            w = [jnp.where(is_high, p[(j + 2) % SPREAD], p[j]) for j in range(SPREAD)]
            for d in range(SPREAD):
                mixed = roll_groups(w[-d % SPREAD], (LANES - d * VB) % LANES)
                row = (db * SPREAD + d) * VB
                for hi in range(blocks):
                    flat[
                        slot,
                        row // (blocks * VB),
                        pl.ds(row % (blocks * VB), VB),
                        hi * LANES : (hi + 1) * LANES,
                    ] = mixed[hi * VB : (hi + 1) * VB, :]

    low = k % 2
    high = k // 2

    def swap_sums(stage, bits, src, dst):
        return pltpu.make_async_remote_copy(
            src_ref=src,
            dst_ref=dst,
            send_sem=csend.at[stage],
            recv_sem=crecv.at[stage],
            device_id={"aux": aux_peer(bits)},
            device_id_type=MESH,
        )

    for stage, side in enumerate((1 - high, high)):
        cols = pl.ds(pl.multiple_of(side * 2 * width, 2 * width), 2 * width)
        total = jnp.zeros((occ, 2 * width), jnp.float32)
        for slot in range(MOST):
            weights = flat[slot, :, :, cols].reshape(pairs, 2 * width)
            term = jnp.dot(
                ampt[plan[2, 0, slot]], weights, preferred_element_type=jnp.float32
            )
            total += jnp.where(slot < counts[0], term, 0.0)
        part[stage, 0] = total[:, :width]
        part[stage, 1] = total[:, width:]
        pair = swap_sums(stage, 1, part.at[stage, 1 - low], inbox.at[stage])
        start(pair)
        if stage == 0:
            pair.wait_recv()
            xsend[...] = (part[stage, low] + inbox[stage]).astype(xsend.dtype)
            far = swap_sums(2, 2, xsend, xin)
            start(far)
        else:
            pair.wait_recv()
            far.wait_recv()
            out[...] = part[stage, low] + inbox[stage] + xin[...].astype(jnp.float32)

    for copy in started:
        copy.wait_send()


def run(factors, amplitudes, counts, plan, n_task, relayed):
    depth, pairs = factors.shape
    occ = amplitudes.shape[0]
    width = pairs // N_AUX
    n_pieces = sum(len(group) for group in cut_rows(depth))
    anywhere = pl.BlockSpec(memory_space=pl.ANY)
    scalars = pl.BlockSpec(memory_space=pltpu.SMEM)
    dma = pltpu.SemaphoreType.DMA
    return pl.pallas_call(
        functools.partial(kernel, n_task, relayed),
        out_shape=jax.ShapeDtypeStruct((occ, width), jnp.float32),
        in_specs=[scalars, scalars, anywhere, anywhere],
        out_specs=pl.BlockSpec(memory_space=pltpu.VMEM),
        scratch_shapes=[
            pltpu.VMEM((SPAN, depth, pairs), jnp.bfloat16),
            pltpu.VMEM((SPAN, occ, pairs), jnp.bfloat16),
            pltpu.VMEM((SPAN, occ, pairs), jnp.bfloat16),
            pltpu.VMEM((2, SPAN, SPREAD, pairs // SPREAD, depth // 2), jnp.bfloat16),
            pltpu.VMEM((2, SPAN, SPREAD, depth // 2, pairs), jnp.bfloat16),
            pltpu.VMEM((MOST, SPREAD, pairs // SPREAD, pairs), jnp.float32),
            pltpu.VMEM((pairs, pairs), jnp.bfloat16),
            pltpu.VMEM((2, 2, occ, width), jnp.float32),
            pltpu.VMEM((2, occ, width), jnp.float32),
            pltpu.VMEM((occ, width), jnp.float32),
            pltpu.VMEM((occ, width), jnp.float32),
            dma((2,)),
            dma((4, n_pieces)),
            dma((SPAN, n_pieces)),
            dma((4,)),
            dma((SPAN,)),
            dma((4, N_AUX - 1)),
            dma((SPAN, N_AUX - 1)),
            dma((3,)),
            dma((3,)),
        ],
        compiler_params=pltpu.CompilerParams(
            vmem_limit_bytes=60 * 1024 * 1024, collective_id=0, has_side_effects=True
        ),
    )(counts, plan, factors, amplitudes)


def solution(mesh):
    n_task, n_aux = mesh.shape["task"], mesh.shape["aux"]
    assert n_aux == N_AUX
    relayed = n_task == 8

    def shards(factors, amplitudes, task_counts, task_tiles):
        plan = jnp.transpose(task_tiles, (2, 0, 1))
        total = run(factors[0], amplitudes[0], task_counts, plan, n_task, relayed)
        return total[None]

    return jax.shard_map(
        shards,
        mesh=mesh,
        in_specs=(P("task", "aux", None), P("task", None, None), P("task"), P("task", None, None)),
        out_specs=P("task", None, "aux"),
        check_vma=False,
    )
```

```python
import functools

import jax
import jax.numpy as jnp
from jax import lax
from jax.experimental import pallas as pl
from jax.experimental.pallas import tpu as pltpu
from jax.sharding import PartitionSpec as P

VB = 32
RADIUS = 2
SPAN = 2 * RADIUS + 1
MOST = 4
LANES = 128
SPREAD = LANES // VB
STEP = 2
N_AUX = 4
MESH = pl.DeviceIdType.MESH


def roll_groups(x, amount):
    if amount == 0:
        return x
    parts = [
        pltpu.roll(x[:, j * LANES : (j + 1) * LANES], amount, 1)
        for j in range(x.shape[1] // LANES)
    ]
    return jnp.concatenate(parts, axis=1)


def cut_rows(depth):
    groups = []
    blocks = depth // LANES
    for b in range(blocks):
        lo = b * LANES
        if b == blocks - 1:
            half = LANES // 2
            groups.append([(lo, half), (lo + half, half)])
        else:
            groups.append([(lo, LANES)])
    return groups


def kernel(n_task, relayed, counts, plan, fac_in, amp_in, out, *scratch):
    depth, pairs = fac_in.shape
    occ = amp_in.shape[0]
    rows = pairs // SPREAD
    body = functools.partial(
        scoped_kernel, n_task, relayed, counts, plan, fac_in, amp_in, out, *scratch
    )
    pl.run_scoped(
        body,
        ampt=pltpu.VMEM((SPAN, occ, pairs), jnp.bfloat16),
        lt=pltpu.VMEM((2, SPAN, SPREAD, rows, depth // 2), jnp.bfloat16),
        right=pltpu.VMEM((2, SPAN, SPREAD, depth // 2, pairs), jnp.bfloat16),
        vacc=pltpu.VMEM((MOST, SPREAD, rows, pairs), jnp.float32),
        swap=pltpu.VMEM((pairs, pairs), jnp.bfloat16),
    )


def scoped_kernel(
    n_task,
    relayed,
    counts,
    plan,
    fac_in,
    amp_in,
    out,
    fac,
    amp,
    part,
    inbox,
    xsend,
    xin,
    local_sem,
    fsend,
    frecv,
    tsend,
    trecv,
    qsend,
    qrecv,
    csend,
    crecv,
    ampt,
    lt,
    right,
    vacc,
    swap,
):
    depth, pairs = fac_in.shape
    occ = amp_in.shape[0]
    share = occ // N_AUX
    blocks = pairs // LANES
    width = pairs // N_AUX
    lanes = STEP * LANES
    t = lax.axis_index("task")
    k = lax.axis_index("aux")
    mate = t + 1 - 2 * (t % 2)
    odd = t % 2

    def aux_peer(bits):
        flip_low = bits % 2
        flip_high = bits // 2
        low = k % 2
        high = k // 2
        if flip_low:
            low = 1 - low
        if flip_high:
            high = 1 - high
        return high * 2 + low

    def wrapped(d):
        return lax.rem(t + d + n_task, n_task)

    if relayed:
        paths = [
            (wrapped(4 * odd - 2), 4 - 4 * odd),
            (mate, 1 + 2 * odd),
            (wrapped(2 - 4 * odd), 4 * odd),
        ]
        ahead, near, behind, late = 4 - 4 * odd, 3 - 2 * odd, 4 * odd, 1 + 2 * odd
        relay_to = 3 - 2 * odd
    else:
        paths = [(wrapped(2), 0), (wrapped(-1), 3), (wrapped(-2), 4), (wrapped(1), 1)]
        ahead, near, behind, late = 0, 3, 4, 1

    barrier = pltpu.get_barrier_semaphore()
    for peer, _ in paths:
        pl.semaphore_signal(barrier, inc=1, device_id={"task": peer}, device_id_type=MESH)
    for bits in range(1, N_AUX):
        pl.semaphore_signal(
            barrier, inc=1, device_id={"aux": aux_peer(bits)}, device_id_type=MESH
        )
    own_f = pltpu.make_async_copy(fac_in, fac.at[RADIUS], local_sem.at[0])
    own_t = pltpu.make_async_copy(amp_in, amp.at[RADIUS], local_sem.at[1])
    own_f.start()
    own_t.start()
    pl.semaphore_wait(barrier, len(paths) + N_AUX - 1)

    groups = cut_rows(depth)
    pieces = [piece for group in groups for piece in group]
    held = depth // 2
    mine = pl.ds(pl.multiple_of(k * share, share), share)

    def send_piece(i, path, peer, src, slot):
        lo, size = pieces[i]
        return pltpu.make_async_remote_copy(
            src_ref=src.at[pl.ds(lo, size)],
            dst_ref=fac.at[slot, pl.ds(lo, size)],
            send_sem=fsend.at[path, i],
            recv_sem=frecv.at[slot, i],
            device_id={"task": peer},
            device_id_type=MESH,
        )

    def send_amp(path, peer, src, slot):
        return pltpu.make_async_remote_copy(
            src_ref=src,
            dst_ref=amp.at[slot, mine],
            send_sem=tsend.at[path],
            recv_sem=trecv.at[slot],
            device_id={"task": peer},
            device_id_type=MESH,
        )

    def spread_amp(slot, order, bits):
        return pltpu.make_async_remote_copy(
            src_ref=amp.at[slot, mine],
            dst_ref=amp.at[slot, mine],
            send_sem=qsend.at[order, bits - 1],
            recv_sem=qrecv.at[slot, bits - 1],
            device_id={"aux": aux_peer(bits)},
            device_id_type=MESH,
        )

    started = []

    def start(copy):
        copy.start()
        started.append(copy)

    def send_own(path):
        peer, slot = paths[path]
        for i in range(len(pieces)):
            start(send_piece(i, path, peer, fac_in, slot))

    for path, (peer, slot) in enumerate(paths):
        start(send_amp(path, peer, amp_in.at[mine], slot))
    send_own(0)
    send_own(1)
    send_own(2)
    if not relayed:
        send_own(3)

    @pl.loop(0, blocks)
    def _(j):
        base = pl.multiple_of(j * LANES, LANES)
        rows = lax.broadcasted_iota(jnp.int32, (LANES, pairs), 0) + base
        cols = lax.broadcasted_iota(jnp.int32, (LANES, pairs), 1)
        hit = rows == (cols % VB) * VB + cols // VB
        swap[pl.ds(base, LANES), :] = hit.astype(jnp.float32).astype(jnp.bfloat16)

    def prepare(slot, b):
        x = fac[slot, pl.ds(b * LANES, LANES), :]
        part_of, lo = b * LANES // held, b * LANES % held
        span = pl.ds(lo, LANES)
        for hi in range(blocks):
            strip = x[:, hi * LANES : (hi + 1) * LANES].T
            for s in range(SPREAD):
                lt[part_of, slot, s, hi * VB : (hi + 1) * VB, span] = strip[
                    s * VB : (s + 1) * VB, :
                ]
        swapped = jnp.dot(x, swap[...], preferred_element_type=jnp.float32)
        for s in range(SPREAD):
            right[part_of, slot, s, span, :] = roll_groups(swapped, s * VB).astype(jnp.bfloat16)

    def prepare_amp(slot):
        ampt[slot] = jnp.dot(
            amp[slot], swap[...], preferred_element_type=jnp.float32
        ).astype(jnp.bfloat16)

    def amp_arrived(slot, order):
        send_amp(0, t, amp_in.at[mine], slot).wait_recv()
        for bits in range(1, N_AUX):
            start(spread_amp(slot, order, bits))

    def amp_ready(slot):
        for bits in range(1, N_AUX):
            spread_amp(slot, 0, bits).wait_recv()
        prepare_amp(slot)

    def arrived(slot, i):
        send_piece(i, 0, t, fac_in, slot).wait_recv()

    own_t.wait()
    own_f.wait()
    prepare_amp(RADIUS)
    for b in range(len(groups)):
        prepare(RADIUS, b)

    amp_arrived(ahead, 0)
    if relayed:
        start(send_amp(3, mate, amp.at[ahead, mine], relay_to))
    amp_arrived(near, 1)
    amp_arrived(behind, 2)

    i = 0
    for b, group in enumerate(groups):
        for _ in group:
            arrived(ahead, i)
            if relayed:
                start(send_piece(i, 3, mate, fac.at[ahead], relay_to))
            i += 1
        prepare(ahead, b)
        for j in range(i - len(group), i):
            arrived(near, j)
        prepare(near, b)
        if b == 0:
            amp_arrived(late, 3)
        if b == 1:
            for slot in (ahead, near, behind, late):
                amp_ready(slot)

    lane_blocks = blocks // STEP

    def product(part_of, slot, s, cols):
        return jnp.dot(
            lt[part_of, plan[0, 0, slot], s],
            right[part_of, plan[1, 0, slot], s, :, cols],
            preferred_element_type=jnp.float32,
        )

    i = 0
    for b, group in enumerate(groups):
        for slot in (behind, late):
            for j in range(i, i + len(group)):
                arrived(slot, j)
            prepare(slot, b)
        i += len(group)
        if (b + 1) * LANES == held:

            @pl.loop(0, MOST)
            def _(slot):
                @pl.loop(0, lane_blocks)
                def _(step):
                    cols = pl.ds(pl.multiple_of(step * lanes, lanes), lanes)
                    for s in range(SPREAD):
                        vacc[slot, s, :, cols] = product(0, slot, s, cols)

    tile = right.at[0]
    height = blocks * VB
    group_of = lax.broadcasted_iota(jnp.int32, (height, LANES), 1) // VB
    is_odd = (group_of % 2).astype(jnp.float32).astype(jnp.bfloat16) > 0.5
    is_high = group_of.astype(jnp.float32).astype(jnp.bfloat16) > 1.5

    @pl.loop(0, MOST)
    def _(slot):
        for step in range(lane_blocks):
            outs = []
            for s in range(SPREAD):
                cols = pl.ds(step * lanes, lanes)
                whole = vacc[slot, s, :, cols] + product(1, slot, s, cols)
                outs.append(whole.astype(jnp.bfloat16))
            for j in range(STEP):
                x = [o[:, j * LANES : (j + 1) * LANES] for o in outs]
                p = [jnp.where(is_odd, x[(n + 1) % SPREAD], x[n]) for n in range(SPREAD)]
                w = [jnp.where(is_high, p[(n + 2) % SPREAD], p[n]) for n in range(SPREAD)]
                for d in range(SPREAD):
                    mixed = w[-d % SPREAD]
                    if d > 0:
                        mixed = pltpu.roll(mixed, LANES - d * VB, 1)
                    row = ((step * STEP + j) * SPREAD + d) * VB
                    at = pl.ds(row % height, VB)
                    for hi in range(blocks):
                        tile[slot, row // height, at, hi * LANES : (hi + 1) * LANES] = mixed[
                            hi * VB : (hi + 1) * VB, :
                        ]

    low = k % 2
    high = k // 2

    def swap_sums(stage, bits, src, dst):
        return pltpu.make_async_remote_copy(
            src_ref=src,
            dst_ref=dst,
            send_sem=csend.at[stage],
            recv_sem=crecv.at[stage],
            device_id={"aux": aux_peer(bits)},
            device_id_type=MESH,
        )

    for stage, side in enumerate((1 - high, high)):
        cols = pl.ds(pl.multiple_of(side * 2 * width, 2 * width), 2 * width)
        total = jnp.zeros((occ, 2 * width), jnp.float32)
        for slot in range(MOST):
            weights = tile[slot, :, :, cols].reshape(pairs, 2 * width)
            term = jnp.dot(
                ampt[plan[2, 0, slot]], weights, preferred_element_type=jnp.float32
            )
            total += jnp.where(slot < counts[0], term, 0.0)
        part[stage, 0] = total[:, :width]
        part[stage, 1] = total[:, width:]
        pair = swap_sums(stage, 1, part.at[stage, 1 - low], inbox.at[stage])
        start(pair)
        if stage == 0:
            pair.wait_recv()
            xsend[...] = (part[stage, low] + inbox[stage]).astype(xsend.dtype)
            far = swap_sums(2, 2, xsend, xin)
            start(far)
        else:
            pair.wait_recv()
            far.wait_recv()
            out[...] = part[stage, low] + inbox[stage] + xin[...].astype(jnp.float32)

    for copy in started:
        copy.wait_send()


def run(factors, amplitudes, counts, plan, n_task, relayed):
    depth, pairs = factors.shape
    occ = amplitudes.shape[0]
    width = pairs // N_AUX
    n_pieces = sum(len(group) for group in cut_rows(depth))
    anywhere = pl.BlockSpec(memory_space=pl.ANY)
    scalars = pl.BlockSpec(memory_space=pltpu.SMEM)
    dma = pltpu.SemaphoreType.DMA
    return pl.pallas_call(
        functools.partial(kernel, n_task, relayed),
        out_shape=jax.ShapeDtypeStruct((occ, width), jnp.float32),
        in_specs=[scalars, scalars, anywhere, anywhere],
        out_specs=pl.BlockSpec(memory_space=pltpu.VMEM),
        scratch_shapes=[
            pltpu.VMEM((SPAN, depth, pairs), jnp.bfloat16),
            pltpu.VMEM((SPAN, occ, pairs), jnp.bfloat16),
            pltpu.VMEM((2, 2, occ, width), jnp.float32),
            pltpu.VMEM((2, occ, width), jnp.float32),
            pltpu.VMEM((occ, width), jnp.float32),
            pltpu.VMEM((occ, width), jnp.float32),
            dma((2,)),
            dma((4, n_pieces)),
            dma((SPAN, n_pieces)),
            dma((4,)),
            dma((SPAN,)),
            dma((4, N_AUX - 1)),
            dma((SPAN, N_AUX - 1)),
            dma((3,)),
            dma((3,)),
        ],
        compiler_params=pltpu.CompilerParams(
            vmem_limit_bytes=60 * 1024 * 1024, collective_id=0, has_side_effects=True
        ),
    )(counts, plan, factors, amplitudes)


def solution(mesh):
    n_task, n_aux = mesh.shape["task"], mesh.shape["aux"]
    assert n_aux == N_AUX
    relayed = n_task == 8

    def shards(factors, amplitudes, task_counts, task_tiles):
        plan = jnp.transpose(task_tiles, (2, 0, 1))
        total = run(factors[0], amplitudes[0], task_counts, plan, n_task, relayed)
        return total[None]

    return jax.shard_map(
        shards,
        mesh=mesh,
        in_specs=(P("task", "aux", None), P("task", None, None), P("task"), P("task", None, None)),
        out_specs=P("task", None, "aux"),
        check_vma=False,
    )
```

```python
import functools

import jax
import jax.numpy as jnp
from jax import lax
from jax.experimental import pallas as pl
from jax.experimental.pallas import tpu as pltpu
from jax.sharding import PartitionSpec as P

VB = 32
RADIUS = 2
SPAN = 2 * RADIUS + 1
MOST = 4
LANES = 128
SPREAD = LANES // VB
STEP = 2
N_AUX = 4
PAIR = 2
MESH = pl.DeviceIdType.MESH


def roll_groups(x, amount):
    if amount == 0:
        return x
    parts = [
        pltpu.roll(x[:, j * LANES : (j + 1) * LANES], amount, 1)
        for j in range(x.shape[1] // LANES)
    ]
    return jnp.concatenate(parts, axis=1)


def cut_rows(depth):
    groups = []
    blocks = depth // LANES
    for b in range(blocks):
        lo = b * LANES
        if b == blocks - 1:
            half = LANES // 2
            groups.append([(lo, half), (lo + half, half)])
        else:
            groups.append([(lo, LANES)])
    return groups


def kernel(n_task, relayed, counts_in, plan_in, fac_in, amp_in, out, *scratch):
    depth, pairs = fac_in.shape
    occ = amp_in.shape[0]
    rows = pairs // SPREAD
    body = functools.partial(
        scoped_kernel, n_task, relayed, counts_in, plan_in, fac_in, amp_in, out, *scratch
    )
    pl.run_scoped(
        body,
        ampt=pltpu.VMEM((SPAN, occ, pairs), jnp.bfloat16),
        lt=pltpu.VMEM((2, SPAN, SPREAD, rows, depth // 2), jnp.bfloat16),
        right_a=pltpu.VMEM((SPAN, SPREAD, depth // 2, pairs), jnp.bfloat16),
        vacc=pltpu.VMEM((MOST, SPREAD, rows, pairs), jnp.float32),
        swap=pltpu.VMEM((pairs, pairs), jnp.bfloat16),
    )


def scoped_kernel(
    n_task,
    relayed,
    counts_in,
    plan_in,
    fac_in,
    amp_in,
    out,
    fac,
    amp,
    right_b,
    part,
    inbox,
    xsend,
    xin,
    counts,
    plan,
    local_sem,
    fsend,
    frecv,
    tsend,
    trecv,
    qsend,
    qrecv,
    csend,
    crecv,
    ampt,
    lt,
    right_a,
    vacc,
    swap,
):
    depth, pairs = fac_in.shape
    occ = amp_in.shape[0]
    share = occ // N_AUX
    blocks = pairs // LANES
    width = pairs // N_AUX
    lanes = STEP * LANES
    t = lax.axis_index("task")
    k = lax.axis_index("aux")
    mate = t + 1 - 2 * (t % 2)
    odd = t % 2

    def aux_peer(bits):
        flip_low = bits % 2
        flip_high = bits // 2
        low = k % 2
        high = k // 2
        if flip_low:
            low = 1 - low
        if flip_high:
            high = 1 - high
        return high * 2 + low

    def wrapped(d):
        return lax.rem(t + d + n_task, n_task)

    if relayed:
        paths = [
            (wrapped(4 * odd - 2), 4 - 4 * odd),
            (mate, 1 + 2 * odd),
            (wrapped(2 - 4 * odd), 4 * odd),
        ]
        ahead, near, behind, late = 4 - 4 * odd, 3 - 2 * odd, 4 * odd, 1 + 2 * odd
        relay_to = 3 - 2 * odd
    else:
        paths = [(wrapped(2), 0), (wrapped(-1), 3), (wrapped(-2), 4), (wrapped(1), 1)]
        ahead, near, behind, late = 0, 3, 4, 1

    barrier = pltpu.get_barrier_semaphore()
    for peer, _ in paths:
        pl.semaphore_signal(barrier, inc=1, device_id={"task": peer}, device_id_type=MESH)
    for bits in range(1, N_AUX):
        pl.semaphore_signal(
            barrier, inc=1, device_id={"aux": aux_peer(bits)}, device_id_type=MESH
        )
    own_f = pltpu.make_async_copy(fac_in, fac.at[RADIUS], local_sem.at[0])
    own_t = pltpu.make_async_copy(amp_in, amp.at[RADIUS], local_sem.at[1])
    own_c = pltpu.make_async_copy(counts_in, counts, local_sem.at[2])
    own_p = pltpu.make_async_copy(plan_in, plan, local_sem.at[3])
    for copy in (own_f, own_t, own_c, own_p):
        copy.start()
    pl.semaphore_wait(barrier, len(paths) + N_AUX - 1)

    groups = cut_rows(depth)
    pieces = [piece for group in groups for piece in group]
    held = depth // 2
    right = (right_a, right_b)
    mine = pl.ds(pl.multiple_of(k * share, share), share)

    def send_piece(i, path, peer, src, slot):
        lo, size = pieces[i]
        return pltpu.make_async_remote_copy(
            src_ref=src.at[pl.ds(lo, size)],
            dst_ref=fac.at[slot, pl.ds(lo, size)],
            send_sem=fsend.at[path, i],
            recv_sem=frecv.at[slot, i],
            device_id={"task": peer},
            device_id_type=MESH,
        )

    def send_amp(path, peer, src, slot):
        return pltpu.make_async_remote_copy(
            src_ref=src,
            dst_ref=amp.at[slot, mine],
            send_sem=tsend.at[path],
            recv_sem=trecv.at[slot],
            device_id={"task": peer},
            device_id_type=MESH,
        )

    def spread_amp(slot, order, bits):
        return pltpu.make_async_remote_copy(
            src_ref=amp.at[slot, mine],
            dst_ref=amp.at[slot, mine],
            send_sem=qsend.at[order, bits - 1],
            recv_sem=qrecv.at[slot, bits - 1],
            device_id={"aux": aux_peer(bits)},
            device_id_type=MESH,
        )

    started = []

    def start(copy):
        copy.start()
        started.append(copy)

    def send_own(path):
        peer, slot = paths[path]
        for i in range(len(pieces)):
            start(send_piece(i, path, peer, fac_in, slot))

    for path, (peer, slot) in enumerate(paths):
        start(send_amp(path, peer, amp_in.at[mine], slot))
    send_own(0)
    send_own(1)
    if not relayed:
        send_own(2)
        send_own(3)

    @pl.loop(0, blocks)
    def _(j):
        base = pl.multiple_of(j * LANES, LANES)
        rows = lax.broadcasted_iota(jnp.int32, (LANES, pairs), 0) + base
        cols = lax.broadcasted_iota(jnp.int32, (LANES, pairs), 1)
        hit = rows == (cols % VB) * VB + cols // VB
        swap[pl.ds(base, LANES), :] = hit.astype(jnp.float32).astype(jnp.bfloat16)

    def prepare(slot, b):
        x = fac[slot, pl.ds(b * LANES, LANES), :]
        part_of, lo = b * LANES // held, b * LANES % held
        span = pl.ds(lo, LANES)
        for hi in range(blocks):
            strip = x[:, hi * LANES : (hi + 1) * LANES].T
            for s in range(SPREAD):
                lt[part_of, slot, s, hi * VB : (hi + 1) * VB, span] = strip[
                    s * VB : (s + 1) * VB, :
                ]
        swapped = jnp.dot(x, swap[...], preferred_element_type=jnp.float32)
        for s in range(SPREAD):
            right[part_of][slot, s, span, :] = roll_groups(swapped, s * VB).astype(jnp.bfloat16)

    def prepare_amp(slot):
        ampt[slot] = jnp.dot(
            amp[slot], swap[...], preferred_element_type=jnp.float32
        ).astype(jnp.bfloat16)

    def amp_arrived(slot, order):
        send_amp(0, t, amp_in.at[mine], slot).wait_recv()
        for bits in range(1, N_AUX):
            start(spread_amp(slot, order, bits))

    def amp_ready(slot):
        for bits in range(1, N_AUX):
            spread_amp(slot, 0, bits).wait_recv()
        prepare_amp(slot)

    def arrived(slot, i):
        send_piece(i, 0, t, fac_in, slot).wait_recv()

    for copy in (own_f, own_t, own_c, own_p):
        copy.wait()
    prepare_amp(RADIUS)
    for b in range(len(groups)):
        prepare(RADIUS, b)

    amp_arrived(ahead, 0)
    if relayed:
        start(send_amp(3, mate, amp.at[ahead, mine], relay_to))
    amp_arrived(near, 1)
    amp_arrived(behind, 2)

    i = 0
    for b, group in enumerate(groups):
        for _ in group:
            arrived(ahead, i)
            if relayed:
                start(send_piece(i, 3, mate, fac.at[ahead], relay_to))
                if i == 3:
                    send_own(2)
            i += 1
        prepare(ahead, b)
        for j in range(i - len(group), i):
            arrived(near, j)
        prepare(near, b)
        if b == 1:
            for slot in (ahead, near, behind):
                amp_ready(slot)

    lane_blocks = blocks // STEP

    def product(part_of, slot, s, cols):
        return jnp.dot(
            lt[part_of, plan[0, 0, slot], s],
            right[part_of][plan[1, 0, slot], s, :, cols],
            preferred_element_type=jnp.float32,
        )

    amp_arrived(late, 3)
    i = 0
    for b, group in enumerate(groups):
        for slot in (behind, late):
            for j in range(i, i + len(group)):
                arrived(slot, j)
            prepare(slot, b)
        i += len(group)
        if b == 0:
            amp_ready(late)
        if (b + 1) * LANES == held:

            @pl.loop(0, MOST)
            def _(slot):
                @pl.loop(0, lane_blocks)
                def _(step):
                    cols = pl.ds(pl.multiple_of(step * lanes, lanes), lanes)
                    for s in range(SPREAD):
                        vacc[slot, s, :, cols] = product(0, slot, s, cols)

    tile = right_a
    height = blocks * VB
    group_of = lax.broadcasted_iota(jnp.int32, (height, LANES), 1) // VB
    is_odd = (group_of % 2).astype(jnp.float32).astype(jnp.bfloat16) > 0.5
    is_high = group_of.astype(jnp.float32).astype(jnp.bfloat16) > 1.5

    def finish(slot):
        for step in range(lane_blocks):
            outs = []
            for s in range(SPREAD):
                cols = pl.ds(step * lanes, lanes)
                whole = vacc[slot, s, :, cols] + product(1, slot, s, cols)
                outs.append(whole.astype(jnp.bfloat16))
            for j in range(STEP):
                x = [o[:, j * LANES : (j + 1) * LANES] for o in outs]
                p = [jnp.where(is_odd, x[(n + 1) % SPREAD], x[n]) for n in range(SPREAD)]
                w = [jnp.where(is_high, p[(n + 2) % SPREAD], p[n]) for n in range(SPREAD)]
                for d in range(SPREAD):
                    mixed = w[-d % SPREAD]
                    if d > 0:
                        mixed = pltpu.roll(mixed, LANES - d * VB, 1)
                    row = ((step * STEP + j) * SPREAD + d) * VB
                    at = pl.ds(row % height, VB)
                    for hi in range(blocks):
                        tile[slot, row // height, at, hi * LANES : (hi + 1) * LANES] = mixed[
                            hi * VB : (hi + 1) * VB, :
                        ]

    @pl.loop(0, MOST // PAIR)
    def _(i):
        for n in range(PAIR):
            finish(i * PAIR + n)

    low = k % 2
    high = k // 2

    def swap_sums(stage, bits, src, dst):
        return pltpu.make_async_remote_copy(
            src_ref=src,
            dst_ref=dst,
            send_sem=csend.at[stage],
            recv_sem=crecv.at[stage],
            device_id={"aux": aux_peer(bits)},
            device_id_type=MESH,
        )

    for stage, side in enumerate((1 - high, high)):
        cols = pl.ds(pl.multiple_of(side * 2 * width, 2 * width), 2 * width)
        total = jnp.zeros((occ, 2 * width), jnp.float32)
        for slot in range(MOST):
            weights = tile[slot, :, :, cols].reshape(pairs, 2 * width)
            term = jnp.dot(
                ampt[plan[2, 0, slot]], weights, preferred_element_type=jnp.float32
            )
            total += jnp.where(slot < counts[0], term, 0.0)
        part[stage, 0] = total[:, :width]
        part[stage, 1] = total[:, width:]
        pair = swap_sums(stage, 1, part.at[stage, 1 - low], inbox.at[stage])
        start(pair)
        if stage == 0:
            pair.wait_recv()
            xsend[...] = (part[stage, low] + inbox[stage]).astype(xsend.dtype)
            far = swap_sums(2, 2, xsend, xin)
            start(far)
        else:
            pair.wait_recv()
            far.wait_recv()
            out[...] = part[stage, low] + inbox[stage] + xin[...].astype(jnp.float32)

    for copy in started:
        copy.wait_send()


def run(factors, amplitudes, counts, plan, n_task, relayed):
    depth, pairs = factors.shape
    occ = amplitudes.shape[0]
    width = pairs // N_AUX
    n_pieces = sum(len(group) for group in cut_rows(depth))
    anywhere = pl.BlockSpec(memory_space=pltpu.HBM)
    dma = pltpu.SemaphoreType.DMA
    return pl.pallas_call(
        functools.partial(kernel, n_task, relayed),
        out_shape=pltpu.VMEM((occ, width), jnp.float32),
        in_specs=[anywhere] * 4,
        out_specs=pl.BlockSpec(memory_space=pltpu.VMEM),
        scratch_shapes=[
            pltpu.VMEM((SPAN, depth, pairs), jnp.bfloat16),
            pltpu.VMEM((SPAN, occ, pairs), jnp.bfloat16),
            pltpu.VMEM((SPAN, SPREAD, depth // 2, pairs), jnp.bfloat16),
            pltpu.VMEM((2, 2, occ, width), jnp.float32),
            pltpu.VMEM((2, occ, width), jnp.float32),
            pltpu.VMEM((occ, width), jnp.float32),
            pltpu.VMEM((occ, width), jnp.float32),
            pltpu.SMEM(counts.shape, jnp.int32),
            pltpu.SMEM(plan.shape, jnp.int32),
            dma((4,)),
            dma((4, n_pieces)),
            dma((SPAN, n_pieces)),
            dma((4,)),
            dma((SPAN,)),
            dma((4, N_AUX - 1)),
            dma((SPAN, N_AUX - 1)),
            dma((3,)),
            dma((3,)),
        ],
        compiler_params=pltpu.CompilerParams(
            vmem_limit_bytes=60 * 1024 * 1024, collective_id=0, has_side_effects=True
        ),
    )(counts, plan, factors, amplitudes)


def solution(mesh):
    n_task, n_aux = mesh.shape["task"], mesh.shape["aux"]
    assert n_aux == N_AUX
    relayed = n_task == 8

    def shards(factors, amplitudes, task_counts, task_tiles):
        plan = jnp.transpose(task_tiles, (2, 0, 1))
        total = run(factors[0], amplitudes[0], task_counts, plan, n_task, relayed)
        return total[None]

    return jax.shard_map(
        shards,
        mesh=mesh,
        in_specs=(P("task", "aux", None), P("task", None, None), P("task"), P("task", None, None)),
        out_specs=P("task", None, "aux"),
        check_vma=False,
    )
```

```python
import functools

import jax
import jax.numpy as jnp
from jax import lax
from jax.experimental import pallas as pl
from jax.experimental.pallas import tpu as pltpu
from jax.sharding import PartitionSpec as P

VB = 32
RADIUS = 2
SPAN = 2 * RADIUS + 1
MOST = 4
LANES = 128
SPREAD = LANES // VB
STEP = 2
N_AUX = 4
PAIR = 2
MESH = pl.DeviceIdType.MESH


def roll_groups(x, amount):
    if amount == 0:
        return x
    parts = [
        pltpu.roll(x[:, j * LANES : (j + 1) * LANES], amount, 1)
        for j in range(x.shape[1] // LANES)
    ]
    return jnp.concatenate(parts, axis=1)


def cut_rows(depth):
    groups = []
    blocks = depth // LANES
    for b in range(blocks):
        lo = b * LANES
        if b == blocks - 1:
            half = LANES // 2
            groups.append([(lo, half), (lo + half, half)])
        else:
            groups.append([(lo, LANES)])
    return groups


def kernel(n_task, relayed, counts_in, plan_in, fac_in, amp_in, out, *scratch):
    depth, pairs = fac_in.shape
    occ = amp_in.shape[0]
    rows = pairs // SPREAD
    body = functools.partial(
        scoped_kernel, n_task, relayed, counts_in, plan_in, fac_in, amp_in, out, *scratch
    )
    pl.run_scoped(
        body,
        ampt=pltpu.VMEM((SPAN, occ, pairs), jnp.bfloat16),
        lt=pltpu.VMEM((2, SPAN, SPREAD, rows, depth // 2), jnp.bfloat16),
        right_a=pltpu.VMEM((SPAN, SPREAD, depth // 2, pairs), jnp.bfloat16),
        vacc=pltpu.VMEM((MOST, SPREAD, rows, pairs), jnp.float32),
        swap=pltpu.VMEM((pairs, pairs), jnp.bfloat16),
    )


def scoped_kernel(
    n_task,
    relayed,
    counts_in,
    plan_in,
    fac_in,
    amp_in,
    out,
    fac,
    amp,
    right_b,
    part,
    inbox,
    xsend,
    xin,
    counts,
    plan,
    local_sem,
    fsend,
    frecv,
    tsend,
    trecv,
    qsend,
    qrecv,
    csend,
    crecv,
    ampt,
    lt,
    right_a,
    vacc,
    swap,
):
    depth, pairs = fac_in.shape
    occ = amp_in.shape[0]
    share = occ // N_AUX
    blocks = pairs // LANES
    width = pairs // N_AUX
    lanes = STEP * LANES
    t = lax.axis_index("task")
    k = lax.axis_index("aux")
    mate = t + 1 - 2 * (t % 2)
    odd = t % 2

    def aux_peer(bits):
        flip_low = bits % 2
        flip_high = bits // 2
        low = k % 2
        high = k // 2
        if flip_low:
            low = 1 - low
        if flip_high:
            high = 1 - high
        return high * 2 + low

    def wrapped(d):
        return lax.rem(t + d + n_task, n_task)

    if relayed:
        paths = [
            (wrapped(4 * odd - 2), 4 - 4 * odd),
            (mate, 1 + 2 * odd),
            (wrapped(2 - 4 * odd), 4 * odd),
        ]
        ahead, near, behind, late = 4 - 4 * odd, 3 - 2 * odd, 4 * odd, 1 + 2 * odd
        relay_to = 3 - 2 * odd
    else:
        paths = [(wrapped(2), 0), (wrapped(-1), 3), (wrapped(-2), 4), (wrapped(1), 1)]
        ahead, near, behind, late = 0, 3, 4, 1

    barrier = pltpu.get_barrier_semaphore()
    for peer, _ in paths:
        pl.semaphore_signal(barrier, inc=1, device_id={"task": peer}, device_id_type=MESH)
    for bits in range(1, N_AUX):
        pl.semaphore_signal(
            barrier, inc=1, device_id={"aux": aux_peer(bits)}, device_id_type=MESH
        )
    own_f = pltpu.make_async_copy(fac_in, fac.at[RADIUS], local_sem.at[0])
    own_t = pltpu.make_async_copy(amp_in, amp.at[RADIUS], local_sem.at[1])
    own_c = pltpu.make_async_copy(counts_in, counts, local_sem.at[2])
    own_p = pltpu.make_async_copy(plan_in, plan, local_sem.at[3])
    for copy in (own_f, own_t, own_c, own_p):
        copy.start()
    pl.semaphore_wait(barrier, len(paths) + N_AUX - 1)

    groups = cut_rows(depth)
    pieces = [piece for group in groups for piece in group]
    held = depth // 2
    right = (right_a, right_b)
    mine = pl.ds(pl.multiple_of(k * share, share), share)

    def send_piece(i, path, peer, src, slot):
        lo, size = pieces[i]
        return pltpu.make_async_remote_copy(
            src_ref=src.at[pl.ds(lo, size)],
            dst_ref=fac.at[slot, pl.ds(lo, size)],
            send_sem=fsend.at[path, i],
            recv_sem=frecv.at[slot, i],
            device_id={"task": peer},
            device_id_type=MESH,
        )

    def send_amp(path, peer, src, slot):
        return pltpu.make_async_remote_copy(
            src_ref=src,
            dst_ref=amp.at[slot, mine],
            send_sem=tsend.at[path],
            recv_sem=trecv.at[slot],
            device_id={"task": peer},
            device_id_type=MESH,
        )

    def spread_amp(slot, order, bits):
        return pltpu.make_async_remote_copy(
            src_ref=amp.at[slot, mine],
            dst_ref=amp.at[slot, mine],
            send_sem=qsend.at[order, bits - 1],
            recv_sem=qrecv.at[slot, bits - 1],
            device_id={"aux": aux_peer(bits)},
            device_id_type=MESH,
        )

    started = []

    def start(copy):
        copy.start()
        started.append(copy)

    def send_own(path):
        peer, slot = paths[path]
        for i in range(len(pieces)):
            start(send_piece(i, path, peer, fac_in, slot))

    for path, (peer, slot) in enumerate(paths):
        start(send_amp(path, peer, amp_in.at[mine], slot))
    send_own(0)
    send_own(1)
    if not relayed:
        send_own(2)
        send_own(3)

    @pl.loop(0, blocks)
    def _(j):
        base = pl.multiple_of(j * LANES, LANES)
        rows = lax.broadcasted_iota(jnp.int32, (LANES, pairs), 0) + base
        cols = lax.broadcasted_iota(jnp.int32, (LANES, pairs), 1)
        hit = rows == (cols % VB) * VB + cols // VB
        swap[pl.ds(base, LANES), :] = hit.astype(jnp.float32).astype(jnp.bfloat16)

    def prepare(slot, b):
        x = fac[slot, pl.ds(b * LANES, LANES), :]
        part_of, lo = b * LANES // held, b * LANES % held
        span = pl.ds(lo, LANES)
        for hi in range(blocks):
            strip = x[:, hi * LANES : (hi + 1) * LANES].T
            for s in range(SPREAD):
                lt[part_of, slot, s, hi * VB : (hi + 1) * VB, span] = strip[
                    s * VB : (s + 1) * VB, :
                ]
        swapped = jnp.dot(x, swap[...], preferred_element_type=jnp.float32)
        for s in range(SPREAD):
            right[part_of][slot, s, span, :] = roll_groups(swapped, s * VB).astype(jnp.bfloat16)

    def prepare_amp(slot):
        ampt[slot] = jnp.dot(
            amp[slot], swap[...], preferred_element_type=jnp.float32
        ).astype(jnp.bfloat16)

    def amp_arrived(slot, order):
        send_amp(0, t, amp_in.at[mine], slot).wait_recv()
        for bits in range(1, N_AUX):
            start(spread_amp(slot, order, bits))

    def amp_ready(slot):
        for bits in range(1, N_AUX):
            spread_amp(slot, 0, bits).wait_recv()
        prepare_amp(slot)

    def arrived(slot, i):
        send_piece(i, 0, t, fac_in, slot).wait_recv()

    for copy in (own_f, own_t, own_c, own_p):
        copy.wait()
    prepare_amp(RADIUS)
    for b in range(len(groups)):
        prepare(RADIUS, b)

    amp_arrived(ahead, 0)
    if relayed:
        start(send_amp(3, mate, amp.at[ahead, mine], relay_to))
    amp_arrived(near, 1)
    amp_arrived(behind, 2)

    i = 0
    for b, group in enumerate(groups):
        for _ in group:
            arrived(ahead, i)
            if relayed:
                start(send_piece(i, 3, mate, fac.at[ahead], relay_to))
                if i == 3:
                    send_own(2)
            i += 1
        prepare(ahead, b)
        for j in range(i - len(group), i):
            arrived(near, j)
        prepare(near, b)
        if b == 1:
            for slot in (ahead, near, behind):
                amp_ready(slot)

    lane_blocks = blocks // STEP

    def product(part_of, slot, s, cols):
        return jnp.dot(
            lt[part_of, plan[0, 0, slot], s],
            right[part_of][plan[1, 0, slot], s, :, cols],
            preferred_element_type=jnp.float32,
        )

    amp_arrived(late, 3)
    i = 0
    for b, group in enumerate(groups):
        for slot in (behind, late):
            for j in range(i, i + len(group)):
                arrived(slot, j)
            prepare(slot, b)
        i += len(group)
        if b == 0:
            amp_ready(late)
        if (b + 1) * LANES == held:

            @pl.loop(0, MOST)
            def _(slot):
                @pl.loop(0, lane_blocks)
                def _(step):
                    cols = pl.ds(pl.multiple_of(step * lanes, lanes), lanes)
                    for s in range(SPREAD):
                        vacc[slot, s, :, cols] = product(0, slot, s, cols)

    tile = right_a
    height = blocks * VB
    group_of = lax.broadcasted_iota(jnp.int32, (height, LANES), 1) // VB
    is_odd = (group_of % 2).astype(jnp.float32).astype(jnp.bfloat16) > 0.5
    is_high = group_of.astype(jnp.float32).astype(jnp.bfloat16) > 1.5

    def finish(slot):
        for step in range(lane_blocks):
            outs = []
            for s in range(SPREAD):
                cols = pl.ds(step * lanes, lanes)
                whole = vacc[slot, s, :, cols] + product(1, slot, s, cols)
                outs.append(whole.astype(jnp.bfloat16))
            for j in range(STEP):
                x = [o[:, j * LANES : (j + 1) * LANES] for o in outs]
                p = [jnp.where(is_odd, x[(n + 1) % SPREAD], x[n]) for n in range(SPREAD)]
                w = [jnp.where(is_high, p[(n + 2) % SPREAD], p[n]) for n in range(SPREAD)]
                for d in range(SPREAD):
                    mixed = w[-d % SPREAD]
                    if d > 0:
                        mixed = pltpu.roll(mixed, LANES - d * VB, 1)
                    row = ((step * STEP + j) * SPREAD + d) * VB
                    at = pl.ds(row % height, VB)
                    for hi in range(blocks):
                        tile[slot, row // height, at, hi * LANES : (hi + 1) * LANES] = mixed[
                            hi * VB : (hi + 1) * VB, :
                        ]

    @pl.loop(0, MOST // PAIR)
    def _(i):
        for n in range(PAIR):
            finish(i * PAIR + n)

    low = k % 2
    high = k // 2

    def swap_sums(stage, bits, src, dst):
        return pltpu.make_async_remote_copy(
            src_ref=src,
            dst_ref=dst,
            send_sem=csend.at[stage],
            recv_sem=crecv.at[stage],
            device_id={"aux": aux_peer(bits)},
            device_id_type=MESH,
        )

    for stage, side in enumerate((1 - high, high)):
        cols = pl.ds(pl.multiple_of(side * 2 * width, 2 * width), 2 * width)
        total = jnp.zeros((occ, 2 * width), jnp.float32)
        for slot in range(MOST):
            weights = tile[slot, :, :, cols].reshape(pairs, 2 * width)
            term = jnp.dot(
                ampt[plan[2, 0, slot]], weights, preferred_element_type=jnp.float32
            )
            total += jnp.where(slot < counts[0], term, 0.0)
        part[stage, 0] = total[:, :width]
        part[stage, 1] = total[:, width:]
        pair = swap_sums(stage, 1, part.at[stage, 1 - low], inbox.at[stage])
        start(pair)
        if stage == 0:
            pair.wait_recv()
            xsend[...] = (part[stage, low] + inbox[stage]).astype(xsend.dtype)
            far = swap_sums(2, 2, xsend, xin)
            start(far)
        else:
            pair.wait_recv()
            far.wait_recv()
            out[...] = part[stage, low] + inbox[stage] + xin[...].astype(jnp.float32)

    for copy in started:
        copy.wait_send()


def run(factors, amplitudes, counts, plan, n_task, relayed):
    depth, pairs = factors.shape
    occ = amplitudes.shape[0]
    width = pairs // N_AUX
    n_pieces = sum(len(group) for group in cut_rows(depth))
    anywhere = pl.BlockSpec(memory_space=pltpu.HBM)
    dma = pltpu.SemaphoreType.DMA
    return pl.pallas_call(
        functools.partial(kernel, n_task, relayed),
        out_shape=pltpu.VMEM((occ, width), jnp.float32),
        in_specs=[anywhere] * 4,
        out_specs=pl.BlockSpec(memory_space=pltpu.VMEM),
        scratch_shapes=[
            pltpu.VMEM((SPAN, depth, pairs), jnp.bfloat16),
            pltpu.VMEM((SPAN, occ, pairs), jnp.bfloat16),
            pltpu.VMEM((SPAN, SPREAD, depth // 2, pairs), jnp.bfloat16),
            pltpu.VMEM((2, 2, occ, width), jnp.float32),
            pltpu.VMEM((2, occ, width), jnp.float32),
            pltpu.VMEM((occ, width), jnp.bfloat16),
            pltpu.VMEM((occ, width), jnp.bfloat16),
            pltpu.SMEM(counts.shape, jnp.int32),
            pltpu.SMEM(plan.shape, jnp.int32),
            dma((4,)),
            dma((4, n_pieces)),
            dma((SPAN, n_pieces)),
            dma((4,)),
            dma((SPAN,)),
            dma((4, N_AUX - 1)),
            dma((SPAN, N_AUX - 1)),
            dma((3,)),
            dma((3,)),
        ],
        compiler_params=pltpu.CompilerParams(
            vmem_limit_bytes=60 * 1024 * 1024, collective_id=0, has_side_effects=True
        ),
    )(counts, plan, factors, amplitudes)


def solution(mesh):
    n_task, n_aux = mesh.shape["task"], mesh.shape["aux"]
    assert n_aux == N_AUX
    relayed = n_task == 8

    def shards(factors, amplitudes, task_counts, task_tiles):
        plan = jnp.transpose(task_tiles, (2, 0, 1))
        total = run(factors[0], amplitudes[0], task_counts, plan, n_task, relayed)
        return total[None]

    return jax.shard_map(
        shards,
        mesh=mesh,
        in_specs=(P("task", "aux", None), P("task", None, None), P("task"), P("task", None, None)),
        out_specs=P("task", None, "aux"),
        check_vma=False,
    )
```

```python
import functools

import jax
import jax.numpy as jnp
from jax import lax
from jax.experimental import pallas as pl
from jax.experimental.pallas import tpu as pltpu
from jax.sharding import PartitionSpec as P

VB = 32
RADIUS = 2
SPAN = 2 * RADIUS + 1
MOST = 4
LANES = 128
SPREAD = LANES // VB
STEP = 2
N_AUX = 4
MESH = pl.DeviceIdType.MESH


def roll_groups(x, amount):
    if amount == 0:
        return x
    parts = [
        pltpu.roll(x[:, j * LANES : (j + 1) * LANES], amount, 1)
        for j in range(x.shape[1] // LANES)
    ]
    return jnp.concatenate(parts, axis=1)


def cut_rows(depth):
    groups = []
    blocks = depth // LANES
    for b in range(blocks):
        lo = b * LANES
        if b == blocks - 1:
            half = LANES // 2
            groups.append([(lo, half), (lo + half, half)])
        else:
            groups.append([(lo, LANES)])
    return groups


def kernel(n_task, relayed, counts_in, plan_in, fac_in, amp_in, out, *scratch):
    depth, pairs = fac_in.shape
    occ = amp_in.shape[0]
    rows = pairs // SPREAD
    body = functools.partial(
        scoped_kernel, n_task, relayed, counts_in, plan_in, fac_in, amp_in, out, *scratch
    )
    pl.run_scoped(
        body,
        ampt=pltpu.VMEM((SPAN, occ, pairs), jnp.bfloat16),
        lt_a=pltpu.VMEM((SPAN, SPREAD, rows, depth // 2), jnp.bfloat16),
        lt_b=pltpu.VMEM((SPAN, SPREAD, rows, depth // 2), jnp.bfloat16),
        right_a=pltpu.VMEM((SPAN, SPREAD, depth // 2, pairs), jnp.bfloat16),
        vacc=pltpu.VMEM((MOST, SPREAD, rows, pairs), jnp.float32),
        swap=pltpu.VMEM((pairs, pairs), jnp.bfloat16),
    )


def scoped_kernel(
    n_task,
    relayed,
    counts_in,
    plan_in,
    fac_in,
    amp_in,
    out,
    fac,
    amp,
    right_b,
    part,
    inbox,
    xsend,
    xin,
    counts,
    plan,
    local_sem,
    fsend,
    frecv,
    tsend,
    trecv,
    qsend,
    qrecv,
    csend,
    crecv,
    ampt,
    lt_a,
    lt_b,
    right_a,
    vacc,
    swap,
):
    depth, pairs = fac_in.shape
    occ = amp_in.shape[0]
    share = occ // N_AUX
    blocks = pairs // LANES
    width = pairs // N_AUX
    lanes = STEP * LANES
    t = lax.axis_index("task")
    k = lax.axis_index("aux")
    mate = t + 1 - 2 * (t % 2)
    odd = t % 2

    def aux_peer(bits):
        flip_low = bits % 2
        flip_high = bits // 2
        low = k % 2
        high = k // 2
        if flip_low:
            low = 1 - low
        if flip_high:
            high = 1 - high
        return high * 2 + low

    def wrapped(d):
        return lax.rem(t + d + n_task, n_task)

    if relayed:
        paths = [
            (wrapped(4 * odd - 2), 4 - 4 * odd),
            (mate, 1 + 2 * odd),
            (wrapped(2 - 4 * odd), 4 * odd),
        ]
        ahead, near, behind, late = 4 - 4 * odd, 3 - 2 * odd, 4 * odd, 1 + 2 * odd
        relay_to = 3 - 2 * odd
    else:
        paths = [(wrapped(2), 0), (wrapped(-1), 3), (wrapped(-2), 4), (wrapped(1), 1)]
        ahead, near, behind, late = 0, 3, 4, 1

    barrier = pltpu.get_barrier_semaphore()
    for peer, _ in paths:
        pl.semaphore_signal(barrier, inc=1, device_id={"task": peer}, device_id_type=MESH)
    for bits in range(1, N_AUX):
        pl.semaphore_signal(
            barrier, inc=1, device_id={"aux": aux_peer(bits)}, device_id_type=MESH
        )
    own_f = pltpu.make_async_copy(fac_in, fac.at[RADIUS], local_sem.at[0])
    own_t = pltpu.make_async_copy(amp_in, amp.at[RADIUS], local_sem.at[1])
    own_c = pltpu.make_async_copy(counts_in, counts, local_sem.at[2])
    own_p = pltpu.make_async_copy(plan_in, plan, local_sem.at[3])
    for copy in (own_f, own_t, own_c, own_p):
        copy.start()
    pl.semaphore_wait(barrier, len(paths) + N_AUX - 1)

    groups = cut_rows(depth)
    pieces = [piece for group in groups for piece in group]
    held = depth // 2
    left = (lt_a, lt_b)
    right = (right_a, right_b)
    mine = pl.ds(pl.multiple_of(k * share, share), share)

    def send_piece(i, path, peer, src, slot):
        lo, size = pieces[i]
        return pltpu.make_async_remote_copy(
            src_ref=src.at[pl.ds(lo, size)],
            dst_ref=fac.at[slot, pl.ds(lo, size)],
            send_sem=fsend.at[path, i],
            recv_sem=frecv.at[slot, i],
            device_id={"task": peer},
            device_id_type=MESH,
        )

    def send_amp(path, peer, src, slot):
        return pltpu.make_async_remote_copy(
            src_ref=src,
            dst_ref=amp.at[slot, mine],
            send_sem=tsend.at[path],
            recv_sem=trecv.at[slot],
            device_id={"task": peer},
            device_id_type=MESH,
        )

    def spread_amp(slot, order, bits):
        return pltpu.make_async_remote_copy(
            src_ref=amp.at[slot, mine],
            dst_ref=amp.at[slot, mine],
            send_sem=qsend.at[order, bits - 1],
            recv_sem=qrecv.at[slot, bits - 1],
            device_id={"aux": aux_peer(bits)},
            device_id_type=MESH,
        )

    started = []

    def start(copy):
        copy.start()
        started.append(copy)

    def send_own(path):
        peer, slot = paths[path]
        for i in range(len(pieces)):
            start(send_piece(i, path, peer, fac_in, slot))

    for path, (peer, slot) in enumerate(paths):
        start(send_amp(path, peer, amp_in.at[mine], slot))
    send_own(0)
    send_own(1)
    if not relayed:
        send_own(2)
        send_own(3)

    @pl.loop(0, blocks)
    def _(j):
        base = pl.multiple_of(j * LANES, LANES)
        rows = lax.broadcasted_iota(jnp.int32, (LANES, pairs), 0) + base
        cols = lax.broadcasted_iota(jnp.int32, (LANES, pairs), 1)
        hit = rows == (cols % VB) * VB + cols // VB
        swap[pl.ds(base, LANES), :] = hit.astype(jnp.float32).astype(jnp.bfloat16)

    def prepare(slots, b):
        part_of, lo = b * LANES // held, b * LANES % held
        span = pl.ds(lo, LANES)
        tiles = [fac[slot, pl.ds(b * LANES, LANES), :] for slot in slots]
        for slot, x in zip(slots, tiles):
            for hi in range(blocks):
                strip = x[:, hi * LANES : (hi + 1) * LANES].T
                for s in range(SPREAD):
                    left[part_of][slot, s, hi * VB : (hi + 1) * VB, span] = strip[
                        s * VB : (s + 1) * VB, :
                    ]
        swapped = jnp.dot(
            jnp.concatenate(tiles, axis=0), swap[...], preferred_element_type=jnp.float32
        )
        for n, slot in enumerate(slots):
            rows = swapped[n * LANES : (n + 1) * LANES, :]
            for s in range(SPREAD):
                right[part_of][slot, s, span, :] = roll_groups(rows, s * VB).astype(jnp.bfloat16)

    def prepare_amp(slot):
        ampt[slot] = jnp.dot(
            amp[slot], swap[...], preferred_element_type=jnp.float32
        ).astype(jnp.bfloat16)

    def amp_arrived(slot, order):
        send_amp(0, t, amp_in.at[mine], slot).wait_recv()
        for bits in range(1, N_AUX):
            start(spread_amp(slot, order, bits))

    def amp_ready(slot):
        for bits in range(1, N_AUX):
            spread_amp(slot, 0, bits).wait_recv()
        prepare_amp(slot)

    def arrived(slot, i):
        send_piece(i, 0, t, fac_in, slot).wait_recv()

    for copy in (own_f, own_t, own_c, own_p):
        copy.wait()
    prepare_amp(RADIUS)
    for b in range(len(groups)):
        prepare([RADIUS], b)

    amp_arrived(ahead, 0)
    if relayed:
        start(send_amp(3, mate, amp.at[ahead, mine], relay_to))
    amp_arrived(near, 1)
    amp_arrived(behind, 2)

    i = 0
    for b, group in enumerate(groups):
        for _ in group:
            arrived(ahead, i)
            if relayed:
                start(send_piece(i, 3, mate, fac.at[ahead], relay_to))
                if i == 3:
                    send_own(2)
            i += 1
        prepare([ahead], b)
        for j in range(i - len(group), i):
            arrived(near, j)
        prepare([near], b)
        if b == 1:
            for slot in (ahead, near, behind):
                amp_ready(slot)

    lane_blocks = blocks // STEP

    def product(part_of, slot, s, rows, cols):
        return jnp.dot(
            left[part_of][plan[0, 0, slot], s, rows],
            right[part_of][plan[1, 0, slot], s, :, cols],
            preferred_element_type=jnp.float32,
        )

    amp_arrived(late, 3)
    i = 0
    for b, group in enumerate(groups):
        for slot in (behind, late):
            for j in range(i, i + len(group)):
                arrived(slot, j)
        prepare([behind, late], b)
        i += len(group)
        if b == 0:
            amp_ready(late)
        if (b + 1) * LANES == held:

            @pl.loop(0, MOST)
            def _(slot):
                @pl.loop(0, lane_blocks)
                def _(step):
                    cols = pl.ds(pl.multiple_of(step * lanes, lanes), lanes)
                    for s in range(SPREAD):
                        vacc[slot, s, :, cols] = product(0, slot, s, slice(None), cols)

    tile = right_a
    height = blocks * VB
    half = height // 2
    group_of = lax.broadcasted_iota(jnp.int32, (half, LANES), 1) // VB
    is_odd = (group_of % 2).astype(jnp.float32).astype(jnp.bfloat16) > 0.5
    is_high = group_of.astype(jnp.float32).astype(jnp.bfloat16) > 1.5

    def finish(side, slot):
        rows = pl.ds(pl.multiple_of(side * half, half), half)
        for step in range(lane_blocks):
            outs = []
            for s in range(SPREAD):
                cols = pl.ds(step * lanes, lanes)
                whole = vacc[slot, s, rows, cols] + product(1, slot, s, rows, cols)
                outs.append(whole.astype(jnp.bfloat16))
            for j in range(STEP):
                x = [o[:, j * LANES : (j + 1) * LANES] for o in outs]
                p = [jnp.where(is_odd, x[(n + 1) % SPREAD], x[n]) for n in range(SPREAD)]
                w = [jnp.where(is_high, p[(n + 2) % SPREAD], p[n]) for n in range(SPREAD)]
                for d in range(SPREAD):
                    mixed = w[-d % SPREAD]
                    if d > 0:
                        mixed = pltpu.roll(mixed, LANES - d * VB, 1)
                    row = ((step * STEP + j) * SPREAD + d) * VB
                    at = pl.ds(row % height, VB)
                    for hi in range(half // VB):
                        base = pl.multiple_of(side * 2 * width + hi * LANES, LANES)
                        tile[slot, row // height, at, pl.ds(base, LANES)] = mixed[
                            hi * VB : (hi + 1) * VB, :
                        ]

    low = k % 2
    high = k // 2

    def swap_sums(stage, bits, src, dst):
        return pltpu.make_async_remote_copy(
            src_ref=src,
            dst_ref=dst,
            send_sem=csend.at[stage],
            recv_sem=crecv.at[stage],
            device_id={"aux": aux_peer(bits)},
            device_id_type=MESH,
        )

    def terms(base, size):
        cols = pl.ds(pl.multiple_of(base, width), size)
        total = jnp.zeros((occ, size), jnp.float32)
        for slot in range(MOST):
            weights = tile[slot, :, pl.ds(0, height), cols].reshape(pairs, size)
            term = jnp.dot(
                ampt[plan[2, 0, slot]], weights, preferred_element_type=jnp.float32
            )
            total += jnp.where(slot < counts[0], term, 0.0)
        return total

    other = 1 - high
    for slot in range(MOST):
        finish(other, slot)
    total = terms(other * 2 * width, 2 * width)
    part[0, 0] = total[:, :width]
    part[0, 1] = total[:, width:]
    pair = swap_sums(0, 1, part.at[0, 1 - low], inbox.at[0])
    start(pair)
    pair.wait_recv()
    xsend[...] = (part[0, low] + inbox[0]).astype(xsend.dtype)
    far = swap_sums(2, 2, xsend, xin)
    start(far)
    for slot in range(MOST):
        finish(high, slot)
    part[1, 0] = terms((high * 2 + 1 - low) * width, width)
    pair = swap_sums(1, 1, part.at[1, 0], inbox.at[1])
    start(pair)
    kept = terms(k * width, width)
    pair.wait_recv()
    kept += inbox[1]
    far.wait_recv()
    out[...] = kept + xin[...].astype(jnp.float32)

    for copy in started:
        copy.wait_send()


def run(factors, amplitudes, counts, plan, n_task, relayed):
    depth, pairs = factors.shape
    occ = amplitudes.shape[0]
    width = pairs // N_AUX
    n_pieces = sum(len(group) for group in cut_rows(depth))
    anywhere = pl.BlockSpec(memory_space=pltpu.HBM)
    dma = pltpu.SemaphoreType.DMA
    return pl.pallas_call(
        functools.partial(kernel, n_task, relayed),
        out_shape=pltpu.VMEM((occ, width), jnp.float32),
        in_specs=[anywhere] * 4,
        out_specs=pl.BlockSpec(memory_space=pltpu.VMEM),
        scratch_shapes=[
            pltpu.VMEM((SPAN, depth, pairs), jnp.bfloat16),
            pltpu.VMEM((SPAN, occ, pairs), jnp.bfloat16),
            pltpu.VMEM((SPAN, SPREAD, depth // 2, pairs), jnp.bfloat16),
            pltpu.VMEM((2, 2, occ, width), jnp.float32),
            pltpu.VMEM((2, occ, width), jnp.float32),
            pltpu.VMEM((occ, width), jnp.bfloat16),
            pltpu.VMEM((occ, width), jnp.bfloat16),
            pltpu.SMEM(counts.shape, jnp.int32),
            pltpu.SMEM(plan.shape, jnp.int32),
            dma((4,)),
            dma((4, n_pieces)),
            dma((SPAN, n_pieces)),
            dma((4,)),
            dma((SPAN,)),
            dma((4, N_AUX - 1)),
            dma((SPAN, N_AUX - 1)),
            dma((3,)),
            dma((3,)),
        ],
        compiler_params=pltpu.CompilerParams(
            vmem_limit_bytes=60 * 1024 * 1024, collective_id=0, has_side_effects=True
        ),
    )(counts, plan, factors, amplitudes)


def solution(mesh):
    n_task, n_aux = mesh.shape["task"], mesh.shape["aux"]
    assert n_aux == N_AUX
    relayed = n_task == 8

    def shards(factors, amplitudes, task_counts, task_tiles):
        plan = jnp.transpose(task_tiles, (2, 0, 1))
        total = run(factors[0], amplitudes[0], task_counts, plan, n_task, relayed)
        return total[None]

    return jax.shard_map(
        shards,
        mesh=mesh,
        in_specs=(P("task", "aux", None), P("task", None, None), P("task"), P("task", None, None)),
        out_specs=P("task", None, "aux"),
        check_vma=False,
    )
```
